8 devices in a mesh: dp: 2 (over z, y), sp: 4 (over x, core).
Axes of the slice: x: 2, y: 2, z: 1, core: 2. Of those that a mesh axis runs over, the one named last changes fastest.
Arguments:
- hidden: bfloat16 [32, 1024, 1024], P('dp', 'sp'), parts along dimension 0
- pos_ids: int32 [32, 1024], P('dp', 'sp'), parts along dimension 0
- block_ids: int32 [32, 1024], P('dp', 'sp'), parts along dimension 0
- ctx_len: int32 [32], P('dp'), parts along dimension 0
- ln_gamma: bfloat16 [1024], replicated
- ln_beta: bfloat16 [1024], replicated
- w_qkv: bfloat16 [1024, 16, 3, 64], replicated
- b_qkv: bfloat16 [16, 3, 64], replicated
- w_dense: bfloat16 [1024, 1024], replicated
- b_dense: bfloat16 [1024], replicated
Outputs:
- output 1: bfloat16 [32, 1024, 1024], P('dp', 'sp'), parts along dimension 0
- output 2: bfloat16 [32, 1024, 16, 64], P('dp', None, 'sp'), parts along dimension 0
- output 3: bfloat16 [32, 1024, 16, 64], P('dp', None, 'sp'), parts along dimension 0
There are 2 independent parts. The reference program is written for one: setup_inputs(seed, part) draws one part's arguments, and reference() takes and returns one part's arrays. A program takes and returns all parts, laid end to end along the dimension named above; an argument that names none is the same for every part.
All inputs are finite; a program needn't handle non-finite values.
Results may differ from the reference program's by a relative error of at most 0.00597672.
Values are sent between devices in bfloat16 or wider.
A program may use at most 1 GiB of HBM per device.

```python
import math
import jax
import jax.numpy as jnp
from jax import lax

BATCH = 16
SEQ = 1024
HEADS = 16
HEAD = 64
HIDDEN = HEADS * HEAD
ALPHA = math.sqrt(56.0)
ROPE_BASE = 10000.0
LN_EPS = 1e-5
SCORE_SCALE = 1.0 / math.sqrt(HEAD)
QUERY_BLOCK = min(SEQ, 128)
GAIN = 1.0 / ALPHA
QKV_SCALE = ALPHA / math.sqrt(HIDDEN)
DENSE_SCALE = 0.5 * math.sqrt(SEQ / HIDDEN)
BIAS_SCALE = 1.0 / math.sqrt(SEQ)


def draw_positions(ctx_key, mask_key):
    ctx_len = jax.random.randint(ctx_key, (BATCH,), SEQ // 4, 3 * SEQ // 4 + 1, dtype=jnp.int32)
    mask_pos = jax.random.randint(mask_key, (BATCH,), 0, ctx_len, dtype=jnp.int32)
    token_pos = jnp.arange(SEQ, dtype=jnp.int32)[None, :]
    in_context = token_pos < ctx_len[:, None]
    pos_ids = jnp.where(in_context, token_pos, mask_pos[:, None]).astype(jnp.int32)
    block_ids = jnp.where(in_context, 0, token_pos - ctx_len[:, None] + 1).astype(jnp.int32)
    return pos_ids, block_ids, ctx_len


def setup_inputs(seed: int = 0, part: int = 0) -> dict:
    base_key = jax.random.key(seed)
    shared_key, part_key = jax.random.split(base_key)
    part_key = jax.random.fold_in(part_key, part)
    key_x, key_ctx, key_mask = jax.random.split(part_key, 3)
    key_g, key_b, key_w, key_wb, key_d, key_db = jax.random.split(shared_key, 6)
    pos_ids, block_ids, ctx_len = draw_positions(key_ctx, key_mask)
    hidden = jax.random.normal(key_x, (BATCH, SEQ, HIDDEN), jnp.float32)
    ln_gamma = (1.0 + 0.2 * jax.random.normal(key_g, (HIDDEN,), jnp.float32)) * GAIN
    ln_beta = jax.random.normal(key_b, (HIDDEN,), jnp.float32) * (GAIN * BIAS_SCALE)
    w_qkv = jax.random.normal(key_w, (HIDDEN, HEADS, 3, HEAD), jnp.float32) * QKV_SCALE
    b_qkv = jax.random.normal(key_wb, (HEADS, 3, HEAD), jnp.float32) * BIAS_SCALE
    w_dense = jax.random.normal(key_d, (HIDDEN, HIDDEN), jnp.float32) * DENSE_SCALE
    b_dense = jax.random.normal(key_db, (HIDDEN,), jnp.float32) * 0.5
    return {'hidden': hidden.astype(jnp.bfloat16), 'pos_ids': pos_ids, 'block_ids': block_ids, 'ctx_len': ctx_len, 'ln_gamma': ln_gamma.astype(jnp.bfloat16), 'ln_beta': ln_beta.astype(jnp.bfloat16), 'w_qkv': w_qkv.astype(jnp.bfloat16), 'b_qkv': b_qkv.astype(jnp.bfloat16), 'w_dense': w_dense.astype(jnp.bfloat16), 'b_dense': b_dense.astype(jnp.bfloat16)}


def layer_norm(hidden, ln_gamma, ln_beta):
    wide_in = hidden.astype(jnp.float32)
    row_mean = jnp.mean(wide_in, axis=-1, keepdims=True)
    centered = wide_in - row_mean
    row_var = jnp.mean(jnp.square(centered), axis=-1, keepdims=True)
    return (centered * lax.rsqrt(row_var + LN_EPS) * ln_gamma.astype(jnp.float32) + ln_beta.astype(jnp.float32)).astype(jnp.bfloat16)


def rotate(heads_in, pos_ids, block_ids):
    half_dim = heads_in.shape[-1] // 2
    quarter_dim = half_dim // 2
    inv_freq = ROPE_BASE ** (-jnp.arange(0, half_dim, 2).astype(jnp.float32) / half_dim)
    angles = jnp.stack([pos_ids, block_ids], axis=-1).astype(jnp.float32)[..., None] * inv_freq
    cos_a = jnp.cos(angles)[:, :, None]
    sin_a = jnp.sin(angles)[:, :, None]
    split_dims = heads_in.astype(jnp.float32).reshape(heads_in.shape[:-1] + (2, 2, quarter_dim))
    low_part = split_dims[..., 0, :]
    high_part = split_dims[..., 1, :]
    new_low = low_part * cos_a - high_part * sin_a
    new_high = high_part * cos_a + low_part * sin_a
    return jnp.stack([new_low, new_high], axis=-2).reshape(heads_in.shape).astype(jnp.bfloat16)


def reference(hidden, pos_ids, block_ids, ctx_len, ln_gamma, ln_beta, w_qkv, b_qkv, w_dense, b_dense):
    normed = layer_norm(hidden, ln_gamma, ln_beta)
    qkv_flat = jnp.dot(normed.reshape(BATCH * SEQ, HIDDEN), w_qkv.reshape(HIDDEN, 3 * HIDDEN), preferred_element_type=jnp.float32)
    qkv_proj = (qkv_flat.reshape(BATCH, SEQ, HEADS, 3, HEAD) + b_qkv.astype(jnp.float32)).astype(jnp.bfloat16)
    query_rot = rotate(qkv_proj[:, :, :, 0], pos_ids, block_ids)
    key_rot = rotate(qkv_proj[:, :, :, 1], pos_ids, block_ids)
    value_heads = qkv_proj[:, :, :, 2]
    key_pos = jnp.arange(SEQ)
    ctx_visible = key_pos[None, None, :] < ctx_len[:, None, None]

    def one_head(head_args):
        q_head, k_head, v_head = head_args
        k_wide = k_head.astype(jnp.float32)
        v_wide = v_head.astype(jnp.float32)

        def one_block(block_idx):
            block_start = block_idx * QUERY_BLOCK
            q_block = lax.dynamic_slice_in_dim(q_head, block_start, QUERY_BLOCK, axis=1).astype(jnp.float32)
            scores = jnp.einsum('bqe,bke->bqk', q_block, k_wide) * SCORE_SCALE
            q_pos = block_start + jnp.arange(QUERY_BLOCK)
            visible = ctx_visible | (key_pos[None, None, :] <= q_pos[None, :, None])
            attn_probs = jax.nn.softmax(jnp.where(visible, scores, -jnp.inf), axis=-1).astype(jnp.bfloat16)
            return jnp.einsum('bqk,bke->bqe', attn_probs.astype(jnp.float32), v_wide).astype(jnp.bfloat16)

        blocks = lax.map(one_block, jnp.arange(SEQ // QUERY_BLOCK))
        return jnp.moveaxis(blocks, 0, 1).reshape(BATCH, SEQ, HEAD)

    head_major = (jnp.moveaxis(query_rot, 2, 0), jnp.moveaxis(key_rot, 2, 0), jnp.moveaxis(value_heads, 2, 0))
    context = lax.map(one_head, head_major)
    context = jnp.moveaxis(context, 0, 2).reshape(BATCH * SEQ, HIDDEN)
    dense_out = jnp.dot(context, w_dense, preferred_element_type=jnp.float32) + b_dense.astype(jnp.float32)
    block_out = (normed.reshape(BATCH * SEQ, HIDDEN).astype(jnp.float32) * ALPHA + dense_out).astype(jnp.bfloat16)
    return block_out.reshape(BATCH, SEQ, HIDDEN), key_rot, value_heads
```

```python
import functools
import math

import jax
import jax.numpy as jnp
from jax import lax
from jax.experimental import pallas as pl
from jax.experimental.pallas import tpu as pltpu
from jax.sharding import PartitionSpec as P

ALPHA = math.sqrt(56.0)
ROPE_BASE = 10000.0
LN_EPS = 1e-5
BF = jnp.bfloat16
F32 = jnp.float32
CHUNKS = (1, 1, 2, 2, 2, 2, 2, 2, 1, 1)


def ln_kernel(x_ref, g_ref, b_ref, o_ref):
    x = x_ref[0].astype(F32)
    mean = jnp.mean(x, axis=-1, keepdims=True)
    cen = x - mean
    var = jnp.mean(cen * cen, axis=-1, keepdims=True)
    o_ref[0] = (cen * lax.rsqrt(var + LN_EPS) * g_ref[...] + b_ref[...]).astype(BF)


def rope(x, cs, scale):
    rows, t = x.shape
    heads = rows // 64
    x = x.reshape(heads, 2, 2, 16, t)
    cos = cs[:32].reshape(1, 2, 16, t)
    sin = cs[32:].reshape(1, 2, 16, t)
    u, w = x[:, :, 0], x[:, :, 1]
    lo = u * cos - w * sin
    hi = w * cos + u * sin
    out = jnp.stack([lo, hi], axis=2).reshape(rows, t).astype(BF)
    if scale != 1.0:
        out = out * jnp.asarray(scale, BF)
    return out


def attn_kernel(heads, row0, *refs):
    (ctx_ref, wq_ref, wk_ref, wv_ref, bias_ref, a0, a1, a2, a3, cs_ref) = refs[:10]
    (k_out, v_out, mine_ref, send_ref, kt, vt, qt, ct) = refs[-8:]
    hd = heads * 64
    s = lax.axis_index("sp")
    c = lax.rem(s, 2)
    x = lax.div(s, 2)
    t = 256
    nt = (((1,), (1,)), ((), ()))
    for k, a_ref in enumerate((a0, a1, a2, a3)):
        blk = 2 * (x if k < 2 else 1 - x) + (c if k % 2 == 0 else 1 - c)
        off = pl.multiple_of(blk * t, t)
        a = a_ref[0]
        cs = cs_ref[0, k]
        kk = lax.dot_general(wk_ref[...], a, nt, preferred_element_type=F32)
        kk = (kk + bias_ref[hd : 2 * hd]).astype(BF).astype(F32)
        kt[:, pl.ds(off, t)] = rope(kk, cs, 1.0)
        vv = lax.dot_general(wv_ref[...], a, nt, preferred_element_type=F32)
        vt[:, pl.ds(off, t)] = (vv + bias_ref[2 * hd :]).astype(BF)
        if k < 2:
            qoff = pl.multiple_of((c if k == 0 else 1 - c) * t, t)
            qq = lax.dot_general(wq_ref[...], a, nt, preferred_element_type=F32)
            qq = (qq + bias_ref[:hd]).astype(BF).astype(F32)
            qt[:, pl.ds(qoff, t)] = rope(qq, cs, 0.125)
    k_out[0] = kt[: hd // 2]
    v_out[0] = vt[: hd // 2]

    ctx = ctx_ref[row0 + pl.program_id(0)]
    jj = lax.broadcasted_iota(jnp.int32, (t, t), 0)
    ii = lax.broadcasted_iota(jnp.int32, (1, t), 1)

    def head(h, carry):
        ho = pl.multiple_of(h * 64, 64)
        for qi, nk in ((0, 3), (1, 4)):
            q = qt[pl.ds(ho, 64), qi * t : (qi + 1) * t]
            lim = jnp.maximum(ii + (x * 2 + qi) * t, ctx - 1)
            st = lax.dot_general(
                kt[pl.ds(ho, 64), : nk * t], q, (((0,), (0,)), ((), ())), preferred_element_type=F32
            )
            parts = [st[:t]]
            for kb in range(1, nk):
                parts.append(jnp.where(jj <= lim - kb * t, st[kb * t : (kb + 1) * t], -jnp.inf))
            m = parts[0]
            for p in parts[1:]:
                m = jnp.maximum(m, p)
            m = jnp.max(m, axis=0, keepdims=True)
            es = [jnp.exp(p - m) for p in parts]
            l = es[0]
            for e in es[1:]:
                l = l + e
            l = jnp.sum(l, axis=0, keepdims=True)
            pb = jnp.concatenate([e.astype(BF) for e in es], axis=0)
            o = jnp.dot(vt[pl.ds(ho, 64), : nk * t], pb, preferred_element_type=F32)
            ct[qi, pl.ds(ho, 64)] = (o * (1.0 / l)).astype(BF)
        return carry

    lax.fori_loop(0, heads, head, 0, unroll=2)
    mine_ref[0] = ct[c]
    send_ref[0] = ct[1 - c]


def dense_kernel(mine_ref, theirs_ref, w_ref, a_ref, b_ref, *rest):
    o_ref = rest[-1]
    half = mine_ref.shape[1]
    tn = (((0,), (0,)), ((), ()))
    o = lax.dot_general(mine_ref[0], w_ref[:half], tn, preferred_element_type=F32)
    o += lax.dot_general(theirs_ref[0], w_ref[half:], tn, preferred_element_type=F32)
    o_ref[0] = (a_ref[0].astype(F32) * ALPHA + o + b_ref[...]).astype(BF)


def solution(mesh):
    sp = mesh.shape["sp"]
    core_swap = [(i, i ^ 1) for i in range(sp)]
    chip_swap = [(i, i ^ 2) for i in range(sp)]
    both_swap = [(i, i ^ 3) for i in range(sp)]

    def local_block(hidden, pos_ids, block_ids, ctx_len, ln_gamma, ln_beta, w_qkv, b_qkv, w_dense, b_dense):
        rows, tok, width = hidden.shape
        all_heads = w_qkv.shape[1]
        heads = all_heads // 2
        hd = heads * 64
        seq = tok * sp
        s = lax.axis_index("sp")
        c = lax.rem(s, 2)
        x = lax.div(s, 2)
        gamma = ln_gamma.astype(F32).reshape(1, width)
        beta = ln_beta.astype(F32).reshape(1, width)

        const = lambda shape: pl.BlockSpec(shape, lambda r: (0,) * len(shape), pipeline_mode=pl.Buffered(1))
        row_blk = lambda start, shape: pl.BlockSpec((1,) + shape, lambda r: (r + start,) + (0,) * len(shape))
        par = pltpu.CompilerParams(dimension_semantics=("arbitrary",))

        starts = [sum(CHUNKS[:i]) for i in range(len(CHUNKS))]

        def ln(start, n):
            return pl.pallas_call(
                ln_kernel,
                grid=(n,),
                in_specs=[row_blk(start, (tok, width)), const((1, width)), const((1, width))],
                out_specs=row_blk(0, (tok, width)),
                out_shape=jax.ShapeDtypeStruct((n, tok, width), BF),
                cost_estimate=pl.CostEstimate(flops=n * tok * width * 10, bytes_accessed=n * tok * width * 4, transcendentals=0),
                compiler_params=par,
                name="ln",
            )(hidden, gamma, beta)

        a_own = [ln(st, n) for st, n in zip(starts, CHUNKS)]
        a_chip = [lax.ppermute(a, "sp", chip_swap) for a in a_own]
        a_core = [lax.ppermute(a, "sp", core_swap) for a in a_own]
        a_both = [lax.ppermute(a, "sp", core_swap) for a in a_chip]

        pos = [pos_ids] + [lax.ppermute(pos_ids, "sp", pm) for pm in (core_swap, chip_swap, both_swap)]
        blk = [2 * (x if k < 2 else 1 - x) + (c if k % 2 == 0 else 1 - c) for k in range(4)]
        tables = []
        inv = ROPE_BASE ** (-jnp.arange(0, 32, 2).astype(F32) / 32)
        for k in range(4):
            i = blk[k] * tok + jnp.arange(tok, dtype=jnp.int32)[None, :]
            block = jnp.maximum(i - ctx_len[:, None] + 1, 0)
            p = jnp.stack([pos[k], block], axis=1).astype(F32)
            ang = p[:, :, None, :] * inv[None, None, :, None]
            tables.append(jnp.stack([jnp.cos(ang), jnp.sin(ang)], axis=1).reshape(rows, 64, tok))
        cs = jnp.stack(tables, axis=1)

        g0 = 2 * x + c
        g1 = 2 * (1 - x) + c
        h0 = 2 * x + (1 - c)
        h1 = 2 * (1 - x) + (1 - c)
        wt = jnp.transpose(w_qkv, (1, 2, 3, 0)).reshape(4, all_heads // 4, 3, 64, width)
        bt = b_qkv.astype(F32).reshape(4, all_heads // 4, 3, 64)
        pick = lambda arr, g: lax.dynamic_index_in_dim(arr, g, 0, keepdims=False)
        wsel = jnp.concatenate([pick(wt, g0), pick(wt, g1)], axis=0)
        bsel = jnp.concatenate([pick(bt, g0), pick(bt, g1)], axis=0)
        wq, wk, wv = [wsel[:, t].reshape(hd, width) for t in range(3)]
        bias = jnp.transpose(bsel, (1, 0, 2)).reshape(3 * hd, 1)
        wd4 = w_dense.reshape(4, width // 4, width)
        wd = jnp.concatenate([pick(wd4, g) for g in (g0, g1, h0, h1)], axis=0)
        bd = b_dense.astype(F32).reshape(1, width)

        keys = vals = out = None
        for i, (st, n) in enumerate(zip(starts, CHUNKS)):
            kv_shape = jax.ShapeDtypeStruct((rows, hd // 2, seq), BF)
            c_shape = jax.ShapeDtypeStruct((n, hd, tok), BF)
            prev = () if keys is None else (keys, vals)
            flops = n * (2 * seq * width * hd * 2 + 2 * tok * 2 * width * hd + heads * 7 * tok * tok * 4 * 256)
            keys, vals, mine, send = pl.pallas_call(
                functools.partial(attn_kernel, heads, st),
                grid=(n,),
                in_specs=[
                    pl.BlockSpec(memory_space=pltpu.SMEM),
                    const((hd, width)),
                    const((hd, width)),
                    const((hd, width)),
                    const((3 * hd, 1)),
                ]
                + [row_blk(0, (tok, width))] * 4
                + [row_blk(st, (4, 64, tok))]
                + [pl.BlockSpec(memory_space=pl.ANY)] * len(prev),
                out_specs=[row_blk(st, (hd // 2, seq))] * 2 + [row_blk(0, (hd, tok))] * 2,
                out_shape=[kv_shape, kv_shape, c_shape, c_shape],
                scratch_shapes=[
                    pltpu.VMEM((hd, seq), BF),
                    pltpu.VMEM((hd, seq), BF),
                    pltpu.VMEM((hd, 2 * tok), BF),
                    pltpu.VMEM((2, hd, tok), BF),
                ],
                input_output_aliases={10: 0, 11: 1} if prev else {},
                cost_estimate=pl.CostEstimate(flops=flops, bytes_accessed=n * 5 * 2**20, transcendentals=0),
                compiler_params=par,
                name="attn",
            )(ctx_len, wq, wk, wv, bias, a_own[i], a_core[i], a_chip[i], a_both[i], cs, *prev)
            theirs = lax.ppermute(send, "sp", core_swap)
            prev = () if out is None else (out,)
            out = pl.pallas_call(
                dense_kernel,
                grid=(n,),
                in_specs=[
                    row_blk(0, (hd, tok)),
                    row_blk(0, (hd, tok)),
                    const((width, width)),
                    row_blk(0, (tok, width)),
                    const((1, width)),
                ]
                + [pl.BlockSpec(memory_space=pl.ANY)] * len(prev),
                out_specs=row_blk(st, (tok, width)),
                out_shape=jax.ShapeDtypeStruct((rows, tok, width), BF),
                input_output_aliases={5: 0} if prev else {},
                cost_estimate=pl.CostEstimate(flops=n * 2 * tok * width * width, bytes_accessed=n * 2 * 2**20, transcendentals=0),
                compiler_params=par,
                name="dense",
            )(mine, theirs, wd, a_own[i], bd, *prev)

        to_out = lambda kv: jnp.transpose(kv.reshape(rows, heads // 2, 64, seq), (0, 3, 1, 2))
        return out, to_out(keys), to_out(vals)

    seq_spec = P("dp", "sp", None)
    row_spec = P("dp", "sp")
    head_spec = P("dp", None, "sp", None)
    rep = P()
    return jax.shard_map(
        local_block,
        mesh=mesh,
        in_specs=(seq_spec, row_spec, row_spec, P("dp"), rep, rep, rep, rep, rep, rep),
        out_specs=(seq_spec, head_spec, head_spec),
        check_vma=False,
    )
```

```python
import functools
import math

import jax
import jax.numpy as jnp
from jax import lax
from jax.experimental import pallas as pl
from jax.experimental.pallas import tpu as pltpu
from jax.sharding import PartitionSpec as P

ALPHA = math.sqrt(56.0)
ROPE_BASE = 10000.0
LN_EPS = 1e-5
BF = jnp.bfloat16
F32 = jnp.float32
T = 256
HALF_HEADS = 8
HD = HALF_HEADS * 64
GRP = HD // 2
CHUNKS = (1, 1, 2, 2, 2, 2, 2, 2, 1, 1)
UNROLL = 4
BIG = 2.0**60
NT = (((1,), (1,)), ((), ()))
TN = (((0,), (0,)), ((), ()))


def place():
    s = lax.axis_index("sp")
    return lax.div(s, 2), lax.rem(s, 2)


def ln_kernel(splits, x_ref, g_ref, b_ref, *o_refs):
    x = x_ref[0].astype(F32)
    mean = jnp.mean(x, axis=-1, keepdims=True)
    cen = x - mean
    var = jnp.mean(cen * cen, axis=-1, keepdims=True)
    g = jnp.concatenate([g_ref[i : i + 1] for i in range(8)], axis=1)
    b = jnp.concatenate([b_ref[i : i + 1] for i in range(8)], axis=1)
    a = (cen * lax.rsqrt(var + LN_EPS) * g + b).astype(BF)
    r = pl.program_id(0)
    for (st, n), o_ref in zip(splits, o_refs):
        if len(splits) == 1:
            o_ref[0] = a
        else:

            @pl.when((r >= st) & (r < st + n))
            def _(o_ref=o_ref):
                o_ref[0] = a


def rope(x, cos, sin):
    rows, t = x.shape
    x = x.reshape(rows // 64, 2, 2, 16, t)
    u, w = x[:, :, 0], x[:, :, 1]
    return jnp.stack([u * cos - w * sin, w * cos + u * sin], axis=2).reshape(rows, t).astype(BF)


def attn_kernel(row0, *refs):
    (_, ctx_ref, mb_ref, w0_ref, w1_ref, b0_ref, b1_ref, tab_ref, a0, a1, a2, a3) = refs[:12]
    (k_out, v_out, mine_ref, send_ref, tok_ref, kt, vt, qt, ct, mask, cs) = refs[-11:]
    x, c = place()
    row = row0 + pl.program_id(0)
    ctx = ctx_ref[row]
    m_pos = mb_ref[row]
    seq = kt.shape[1]

    tab = tab_ref[...]
    lane = lax.broadcasted_iota(jnp.int32, (1, seq), 1)
    inside = lane < ctx
    at_m = pltpu.roll(tab, lax.rem(seq - m_pos, seq), 1)[:, :1]
    cs[0] = jnp.where(inside, tab, at_m)
    tail = pltpu.roll(tab, ctx - 1, 1)
    cs[1] = jnp.where(inside, jnp.where(lax.broadcasted_iota(jnp.int32, (32, 1), 0) < 16, 1.0, 0.0), tail)

    def w_part(t0, t1):
        return jnp.concatenate(
            [w[0].reshape(4, 192, 1024)[:, t0 * 64 : t1 * 64].reshape(4 * 64 * (t1 - t0), 1024) for w in (w0_ref, w1_ref)],
            axis=0,
        )

    def b_part(t):
        b = jnp.concatenate(
            [b[0].reshape(4, 192, 128)[:, t * 64 : t * 64 + 64].reshape(GRP, 128) for b in (b0_ref, b1_ref)], axis=0
        )
        return jnp.concatenate([b, b], axis=1)

    for k, a_ref in enumerate((a0, a1, a2, a3)):
        blk = 2 * (x if k < 2 else 1 - x) + (c if k % 2 == 0 else 1 - c)
        off = pl.multiple_of(blk * T, T)
        a = a_ref[0]
        cos = jnp.stack([cs[0, :16, pl.ds(off, T)], cs[1, :16, pl.ds(off, T)]], axis=0)[None]
        sin = jnp.stack([cs[0, 16:, pl.ds(off, T)], cs[1, 16:, pl.ds(off, T)]], axis=0)[None]
        kk = lax.dot_general(w_part(1, 2), a, NT, preferred_element_type=F32)
        kt[:, pl.ds(off, T)] = rope((kk + b_part(1)).astype(BF).astype(F32), cos, sin)
        vv = lax.dot_general(w_part(2, 3), a, NT, preferred_element_type=F32)
        vt[:, pl.ds(off, T)] = (vv + b_part(2)).astype(BF)
        if k < 2:
            qoff = pl.multiple_of((c if k == 0 else 1 - c) * T, T)
            qq = lax.dot_general(w_part(0, 1), a, NT, preferred_element_type=F32)
            qq = rope((qq + b_part(0)).astype(BF).astype(F32), cos, sin)
            qt[:, pl.ds(qoff, T)] = qq * jnp.asarray(0.125, BF)
    k_out[0] = kt[:GRP]
    v_out[0] = vt[:GRP]

    jj = lax.broadcasted_iota(jnp.int32, (T, 2 * T), 0)
    lim = jnp.maximum(lax.broadcasted_iota(jnp.int32, (1, 2 * T), 1) + x * (2 * T), ctx - 1)
    for kb in (1, 2, 3):
        mask[kb - 1] = jnp.where(jj <= lim - kb * T, 0.0, -jnp.inf)

    def scores(ho, kb):
        k_blk = kt[pl.ds(ho, 64), kb * T : (kb + 1) * T]
        q = qt[pl.ds(ho, 64), :] if kb < 3 else qt[pl.ds(ho, 64), T:]
        st = lax.dot_general(k_blk, q, TN, preferred_element_type=F32)
        if kb == 0:
            return st
        return st + (mask[kb - 1] if kb < 3 else mask[2, :, T:])

    def finish(ho, es, l):
        pa = jnp.concatenate([e[:, :T] for e in es[:3]], axis=0)
        pb = jnp.concatenate([e[:, T:] for e in es[:3]] + [es[3]], axis=0)
        oa = jnp.dot(vt[pl.ds(ho, 64), : 3 * T], pa, preferred_element_type=F32)
        ob = jnp.dot(vt[pl.ds(ho, 64), :], pb, preferred_element_type=F32)
        inv = 1.0 / l
        ct[0, pl.ds(ho, 64)] = (oa * inv[:, :T]).astype(BF)
        ct[1, pl.ds(ho, 64)] = (ob * inv[:, T:]).astype(BF)
        return oa, ob

    def total(es):
        l = jnp.sum(es[0], axis=0, keepdims=True)
        for e in es[1:3]:
            l = l + jnp.sum(e, axis=0, keepdims=True)
        return jnp.concatenate([l[:, :T], l[:, T:] + jnp.sum(es[3], axis=0, keepdims=True)], axis=1)

    def fast(i, good):
        for u in range(UNROLL):
            ho = pl.multiple_of(i * (UNROLL * 64) + u * 64, 64)
            es = [jnp.exp(scores(ho, kb)) for kb in range(4)]
            l = total(es)
            oa, ob = finish(ho, [e.astype(BF) for e in es], l)
            top = jnp.concatenate(
                [jnp.max(jnp.abs(oa), axis=0, keepdims=True), jnp.max(jnp.abs(ob), axis=0, keepdims=True)], axis=1
            )
            ok = (l >= 1.0 / BIG) & (l <= BIG) & (top <= BIG * BIG)
            good = jnp.minimum(good, jnp.where(ok, 1.0, 0.0))
        return good

    good = lax.fori_loop(0, HALF_HEADS // UNROLL, fast, jnp.ones((1, 2 * T), F32))

    @pl.when(jnp.min(good) < 0.5)
    def _():
        def slow(h, carry):
            ho = pl.multiple_of(h * 64, 64)
            ss = [scores(ho, kb) for kb in range(4)]
            m = jnp.max(ss[0], axis=0, keepdims=True)
            for st in ss[1:3]:
                m = jnp.maximum(m, jnp.max(st, axis=0, keepdims=True))
            mb = jnp.maximum(m[:, T:], jnp.max(ss[3], axis=0, keepdims=True))
            m = jnp.concatenate([m[:, :T], mb], axis=1)
            es = [jnp.exp(st - m) for st in ss[:3]] + [jnp.exp(ss[3] - mb)]
            finish(ho, [e.astype(BF) for e in es], total(es))
            return carry

        lax.fori_loop(0, HALF_HEADS, slow, 0)

    mine_ref[0] = ct[c]
    send_ref[0] = ct[1 - c]
    tok_ref[...] = jnp.zeros_like(tok_ref)


def dense_kernel(mine_ref, theirs_ref, w_ref, a_ref, b_ref, *rest):
    o_ref, tok_ref = rest[-2:]
    x, c = place()
    groups = (2 * x + c, 2 * (1 - x) + c, 2 * x + 1 - c, 2 * (1 - x) + 1 - c)
    w = jnp.concatenate([w_ref[g] for g in groups], axis=0)
    ctx = jnp.concatenate([mine_ref[0], theirs_ref[0]], axis=0)
    b = jnp.concatenate([b_ref[i : i + 1] for i in range(8)], axis=1)
    o = lax.dot_general(ctx, w, TN, preferred_element_type=F32)
    o_ref[0] = (a_ref[0].astype(F32) * ALPHA + o + b).astype(BF)
    tok_ref[...] = jnp.zeros_like(tok_ref)


def solution(mesh):
    sp = mesh.shape["sp"]
    core_swap = [(i, i ^ 1) for i in range(sp)]
    chip_swap = [(i, i ^ 2) for i in range(sp)]
    both_swap = [(i, i ^ 3) for i in range(sp)]

    def local_block(hidden, pos_ids, block_ids, ctx_len, ln_gamma, ln_beta, w_qkv, b_qkv, w_dense, b_dense):
        rows, tok, width = hidden.shape
        seq = tok * sp
        s = lax.axis_index("sp")
        gamma = ln_gamma.astype(F32).reshape(8, width // 8)
        beta = ln_beta.astype(F32).reshape(8, width // 8)
        starts = [sum(CHUNKS[:i]) for i in range(len(CHUNKS))]
        nch = len(CHUNKS)

        whole = pl.BlockSpec(memory_space=pltpu.VMEM)
        any_ = pl.BlockSpec(memory_space=pl.ANY)
        smem = pl.BlockSpec(memory_space=pltpu.SMEM)
        row_blk = lambda start, shape: pl.BlockSpec((1,) + shape, lambda r, *_: (r + start,) + (0,) * len(shape))
        group_blk = lambda j, shape: pl.BlockSpec(
            (1,) + shape, lambda r, g: (g[j],) + (0,) * len(shape), pipeline_mode=pl.Buffered(1)
        )
        par = pltpu.CompilerParams(dimension_semantics=("arbitrary",), vmem_limit_bytes=67_000_000)
        tok_shape = jax.ShapeDtypeStruct((8, 128), F32)
        tok_spec = pl.BlockSpec((8, 128), lambda r, *_: (0, 0))

        def ln(start, sizes):
            n = sum(sizes)
            splits = [(sum(sizes[:i]), sz) for i, sz in enumerate(sizes)]
            return pl.pallas_call(
                functools.partial(ln_kernel, splits),
                grid=(n,),
                in_specs=[row_blk(start, (tok, width)), whole, whole],
                out_specs=[
                    pl.BlockSpec((1, tok, width), lambda r, st=st, sz=sz: (jnp.clip(r - st, 0, sz - 1), 0, 0))
                    for st, sz in splits
                ],
                out_shape=[jax.ShapeDtypeStruct((sz, tok, width), BF) for sz in sizes],
                cost_estimate=pl.CostEstimate(flops=n * tok * width * 10, bytes_accessed=n * tok * width * 4, transcendentals=0),
                compiler_params=pltpu.CompilerParams(dimension_semantics=("arbitrary",), vmem_limit_bytes=67_000_000),
                name="ln",
            )(hidden, gamma, beta)

        a_own = ln(0, CHUNKS[:1]) + ln(starts[1], CHUNKS[1:])
        a_chip = [lax.ppermute(a, "sp", chip_swap) for a in a_own]
        a_core = [lax.ppermute(a, "sp", core_swap) for a in a_own]

        last = pos_ids[:, tok - 1]
        got = [last] + [lax.ppermute(last, "sp", pm) for pm in (core_swap, chip_swap, both_swap)]
        m_pos = got[0]
        for k in (1, 2, 3):
            m_pos = jnp.where((s ^ k) == sp - 1, got[k], m_pos)

        inv = ROPE_BASE ** (-jnp.arange(0, 32, 2).astype(F32) / 32)
        ang = jnp.arange(seq, dtype=jnp.int32).astype(F32)[None, :] * inv[:, None]
        tab = jnp.concatenate([jnp.cos(ang), jnp.sin(ang)], axis=0)

        wt = jnp.transpose(w_qkv, (1, 2, 3, 0)).reshape(4, 3 * GRP, width)
        bias = jnp.broadcast_to(b_qkv.astype(F32).reshape(4, 3 * GRP, 1), (4, 3 * GRP, 128))
        wd = w_dense.reshape(4, GRP, width)
        bd = b_dense.astype(F32).reshape(8, width // 8)

        xc = (lax.div(s, 2), lax.rem(s, 2))
        groups = jnp.stack([2 * xc[0] + xc[1], 2 * (1 - xc[0]) + xc[1]]).astype(jnp.int32)

        keys = vals = out = None
        mine, theirs, dtok = [], [], []

        def dense(i, out):
            n, st = CHUNKS[i], starts[i]
            prev = () if out is None else (out,)
            return pl.pallas_call(
                dense_kernel,
                grid=(n,),
                in_specs=[row_blk(0, (HD, tok)), row_blk(0, (HD, tok)), whole, row_blk(0, (tok, width)), whole]
                + [any_] * len(prev),
                out_specs=[row_blk(st, (tok, width)), tok_spec],
                out_shape=[jax.ShapeDtypeStruct((rows, tok, width), BF), tok_shape],
                input_output_aliases={5: 0} if prev else {},
                cost_estimate=pl.CostEstimate(flops=n * 2 * tok * width * width, bytes_accessed=n * 2 * 2**20, transcendentals=0),
                compiler_params=par,
                name="dense",
            )(mine[i], theirs[i], wd, a_own[i], bd, *prev)

        for i, (st, n) in enumerate(zip(starts, CHUNKS)):
            a_in = a_chip[i]
            a_both = lax.ppermute(a_in, "sp", core_swap)
            if i >= 2:
                out, t = dense(i - 2, out)
                dtok.append(t)
            extra = [] if keys is None else [keys, vals]
            n_alias = len(extra)
            if dtok:
                extra.append(dtok[-1])
            kv_shape = jax.ShapeDtypeStruct((rows, GRP, seq), BF)
            c_shape = jax.ShapeDtypeStruct((n, HD, tok), BF)
            flops = n * (2 * seq * width * HD * 2 + 2 * tok * 2 * width * HD + HALF_HEADS * 7 * tok * tok * 4 * 256)
            keys, vals, own, send, t = pl.pallas_call(
                functools.partial(attn_kernel, st),
                grid_spec=pltpu.PrefetchScalarGridSpec(
                    num_scalar_prefetch=1,
                    grid=(n,),
                    in_specs=[smem, smem]
                    + [group_blk(j, (3 * GRP, width)) for j in (0, 1)]
                    + [group_blk(j, (3 * GRP, 128)) for j in (0, 1)]
                    + [whole]
                    + [row_blk(0, (tok, width))] * 4
                    + [any_] * len(extra),
                    out_specs=[row_blk(st, (GRP, seq))] * 2 + [row_blk(0, (HD, tok))] * 2 + [tok_spec],
                    scratch_shapes=[
                        pltpu.VMEM((HD, seq), BF),
                        pltpu.VMEM((HD, seq), BF),
                        pltpu.VMEM((HD, 2 * tok), BF),
                        pltpu.VMEM((2, HD, tok), BF),
                        pltpu.VMEM((3, tok, 2 * tok), F32),
                        pltpu.VMEM((2, 32, seq), F32),
                    ],
                ),
                out_shape=[kv_shape, kv_shape, c_shape, c_shape, tok_shape],
                input_output_aliases={12: 0, 13: 1} if n_alias else {},
                cost_estimate=pl.CostEstimate(flops=flops, bytes_accessed=n * 5 * 2**20, transcendentals=0),
                compiler_params=par,
                name="attn",
            )(groups, ctx_len, m_pos, wt, wt, bias, bias, tab, a_own[i], a_core[i], a_in, a_both, *extra)
            mine.append(own)
            theirs.append(lax.ppermute(send, "sp", core_swap))

        out, _ = dense(nch - 2, out)
        out, _ = dense(nch - 1, out)
        to_out = lambda kv: jnp.transpose(kv.reshape(rows, HALF_HEADS // 2, 64, seq), (0, 3, 1, 2))
        return out, to_out(keys), to_out(vals)

    seq_spec = P("dp", "sp", None)
    row_spec = P("dp", "sp")
    head_spec = P("dp", None, "sp", None)
    rep = P()
    return jax.shard_map(
        local_block,
        mesh=mesh,
        in_specs=(seq_spec, row_spec, row_spec, P("dp"), rep, rep, rep, rep, rep, rep),
        out_specs=(seq_spec, head_spec, head_spec),
        check_vma=False,
    )
```

```python
import functools
import math

import jax
import jax.numpy as jnp
from jax import lax
from jax.experimental import pallas as pl
from jax.experimental.pallas import tpu as pltpu
from jax.sharding import PartitionSpec as P

ALPHA = math.sqrt(56.0)
ROPE_BASE = 10000.0
LN_EPS = 1e-5
BF = jnp.bfloat16
F32 = jnp.float32
T = 256
HALF_HEADS = 8
HD = HALF_HEADS * 64
GRP = HD // 2
CHUNKS = (1, 2, 2, 2, 2, 2, 2, 2, 1)
UNROLL = 4
BIG = 2.0**60
NT = (((1,), (1,)), ((), ()))
TN = (((0,), (0,)), ((), ()))


def place():
    s = lax.axis_index("sp")
    return lax.div(s, 2), lax.rem(s, 2)


def ln_kernel(splits, x_ref, g_ref, b_ref, *o_refs):
    x = x_ref[0].astype(F32)
    mean = jnp.mean(x, axis=-1, keepdims=True)
    cen = x - mean
    var = jnp.mean(cen * cen, axis=-1, keepdims=True)
    g = jnp.concatenate([g_ref[i : i + 1] for i in range(8)], axis=1)
    b = jnp.concatenate([b_ref[i : i + 1] for i in range(8)], axis=1)
    a = (cen * lax.rsqrt(var + LN_EPS) * g + b).astype(BF)
    r = pl.program_id(0)
    for (st, n), o_ref in zip(splits, o_refs):
        if len(splits) == 1:
            o_ref[0] = a
        else:

            @pl.when((r >= st) & (r < st + n))
            def _(o_ref=o_ref):
                o_ref[0] = a


def rope(x, cos, sin):
    rows, t = x.shape
    x = x.reshape(rows // 64, 2, 2, 16, t)
    u, w = x[:, :, 0], x[:, :, 1]
    return jnp.stack([u * cos - w * sin, w * cos + u * sin], axis=2).reshape(rows, t).astype(BF)


def dense_row(ctx, w, a, b):
    o = lax.dot_general(ctx, w, TN, preferred_element_type=F32)
    return (a.astype(F32) * ALPHA + o + b).astype(BF)


def bias_row(b_ref):
    return jnp.concatenate([b_ref[i : i + 1] for i in range(8)], axis=1)


def attn_kernel(row0, n, prow0, pn, *refs):
    (ctx_ref, mb_ref, tab_ref, bd_ref, wt_hbm, bias_hbm, wd_hbm, a0, a1, a2, a3) = refs[:11]
    pm_hbm, pt_hbm, pa_hbm = refs[11:14] if pn else (None,) * 3
    (k_hbm, v_hbm, mine_hbm, send_hbm, o_hbm) = refs[-27:-22]
    (w, bias, wd, abuf, kt, vt, qt, ct, mask, cs, dctx, da, do) = refs[-22:-9]
    (w_sem, b_sem, wd_sem, a_sem, kv_sem, ct_sem, dc_sem, da_sem, do_sem) = refs[-9:]
    x, c = place()
    seq = kt.shape[1]
    g = (2 * x + c, 2 * (1 - x) + c)
    dg = g + (2 * x + 1 - c, 2 * (1 - x) + 1 - c)
    copy = pltpu.make_async_copy

    def a_copy(r, k):
        slot = lax.rem(r, 2)
        return copy((a0, a1, a2, a3)[k].at[r], abuf.at[slot, k], a_sem.at[slot, k])

    w_copy = [copy(wt_hbm.at[g[j]], w.at[j], w_sem.at[j]) for j in (0, 1)]
    b_copy = [copy(bias_hbm.at[g[j]], bias.at[j], b_sem.at[j]) for j in (0, 1)]
    wd_copy = [copy(wd_hbm.at[dg[j]], wd.at[pl.ds(j * GRP, GRP)], wd_sem.at[j]) for j in range(4)]

    def kv_copy(r):
        return (
            copy(kt.at[pl.ds(0, GRP)], k_hbm.at[row0 + r], kv_sem.at[0]),
            copy(vt.at[pl.ds(0, GRP)], v_hbm.at[row0 + r], kv_sem.at[1]),
        )

    def ct_copy(r):
        return (
            copy(ct.at[c], mine_hbm.at[r], ct_sem.at[0]),
            copy(ct.at[1 - c], send_hbm.at[r], ct_sem.at[1]),
        )

    def d_copy(r):
        return (
            copy(pm_hbm.at[r], dctx.at[r, pl.ds(0, HD)], dc_sem.at[r, 0]),
            copy(pt_hbm.at[r], dctx.at[r, pl.ds(HD, HD)], dc_sem.at[r, 1]),
            copy(pa_hbm.at[r], da.at[r], da_sem.at[r]),
        )

    def o_copy(r):
        return copy(do.at[r], o_hbm.at[prow0 + r], do_sem.at[r])

    a_copy(0, 0).start()
    w_copy[0].start()
    b_copy[0].start()
    w_copy[1].start()
    b_copy[1].start()
    for k in (1, 2, 3):
        a_copy(0, k).start()
    if pn:
        for cp in wd_copy:
            cp.start()
        for r in range(pn):
            for cp in d_copy(r):
                cp.start()

    tab = tab_ref[...]
    lane = lax.broadcasted_iota(jnp.int32, (1, seq), 1)
    is_cos = lax.broadcasted_iota(jnp.int32, (32, 1), 0) < 16
    jj = lax.broadcasted_iota(jnp.int32, (T, 2 * T), 0)
    ii = lax.broadcasted_iota(jnp.int32, (1, 2 * T), 1)

    def project(r, k, first):
        own = k < 2
        blk = 2 * (x if own else 1 - x) + (c if k % 2 == 0 else 1 - c)
        off = pl.multiple_of(blk * T, T)
        a_copy(r, k).wait()
        a = abuf[lax.rem(r, 2), k]
        cos = jnp.stack([cs[0, :16, pl.ds(off, T)], cs[1, :16, pl.ds(off, T)]], axis=0)[None]
        sin = jnp.stack([cs[0, 16:, pl.ds(off, T)], cs[1, 16:, pl.ds(off, T)]], axis=0)[None]
        t0 = 0 if own else 1
        for j in (0, 1):
            if first and k == 0:

                @pl.when(r == 0)
                def _():
                    w_copy[j].wait()
                    b_copy[j].wait()

            wj = w[j].reshape(4, 192, 1024)[:, t0 * 64 :].reshape(4 * 64 * (3 - t0), 1024)
            bj = bias[j].reshape(4, 192, 128)[:, t0 * 64 :].reshape(4 * 64 * (3 - t0), 128)
            z = lax.dot_general(wj, a, NT, preferred_element_type=F32)
            z = (z + jnp.concatenate([bj, bj], axis=1)).astype(BF).reshape(4, 3 - t0, 64, T)
            pick = lambda t: z[:, t - t0].reshape(GRP, T)
            hs = pl.ds(j * GRP, GRP)
            kt[hs, pl.ds(off, T)] = rope(pick(1).astype(F32), cos, sin)
            vt[hs, pl.ds(off, T)] = pick(2)
            if own:
                qoff = pl.multiple_of((c if k == 0 else 1 - c) * T, T)
                qt[hs, pl.ds(qoff, T)] = rope(pick(0).astype(F32), cos, sin) * jnp.asarray(0.125, BF)

    def scores(ho, kb):
        k_blk = kt[pl.ds(ho, 64), kb * T : (kb + 1) * T]
        q = qt[pl.ds(ho, 64), :] if kb < 3 else qt[pl.ds(ho, 64), T:]
        st = lax.dot_general(k_blk, q, TN, preferred_element_type=F32)
        if kb == 0:
            return st
        return st + (mask[kb - 1] if kb < 3 else mask[2, :, T:])

    def finish(ho, es, l):
        pa = jnp.concatenate([e[:, :T] for e in es[:3]], axis=0)
        pb = jnp.concatenate([e[:, T:] for e in es[:3]] + [es[3]], axis=0)
        oa = jnp.dot(vt[pl.ds(ho, 64), : 3 * T], pa, preferred_element_type=F32)
        ob = jnp.dot(vt[pl.ds(ho, 64), :], pb, preferred_element_type=F32)
        inv = 1.0 / l
        ct[0, pl.ds(ho, 64)] = (oa * inv[:, :T]).astype(BF)
        ct[1, pl.ds(ho, 64)] = (ob * inv[:, T:]).astype(BF)
        return oa, ob

    def total(es):
        l = jnp.sum(es[0], axis=0, keepdims=True)
        for e in es[1:3]:
            l = l + jnp.sum(e, axis=0, keepdims=True)
        return jnp.concatenate([l[:, :T], l[:, T:] + jnp.sum(es[3], axis=0, keepdims=True)], axis=1)

    def fast(i, good):
        for u in range(UNROLL):
            ho = pl.multiple_of(i * (UNROLL * 64) + u * 64, 64)
            es = [jnp.exp(scores(ho, kb)) for kb in range(4)]
            l = total(es)
            oa, ob = finish(ho, [e.astype(BF) for e in es], l)
            top = jnp.concatenate(
                [jnp.max(jnp.abs(oa), axis=0, keepdims=True), jnp.max(jnp.abs(ob), axis=0, keepdims=True)], axis=1
            )
            ok = (l >= 1.0 / BIG) & (l <= BIG) & (top <= BIG * BIG)
            good = jnp.minimum(good, jnp.where(ok, 1.0, 0.0))
        return good

    def slow(h, carry):
        ho = pl.multiple_of(h * 64, 64)
        ss = [scores(ho, kb) for kb in range(4)]
        m = jnp.max(ss[0], axis=0, keepdims=True)
        for st in ss[1:3]:
            m = jnp.maximum(m, jnp.max(st, axis=0, keepdims=True))
        mb = jnp.maximum(m[:, T:], jnp.max(ss[3], axis=0, keepdims=True))
        m = jnp.concatenate([m[:, :T], mb], axis=1)
        es = [jnp.exp(st - m) for st in ss[:3]] + [jnp.exp(ss[3] - mb)]
        finish(ho, [e.astype(BF) for e in es], total(es))
        return carry

    def row(r, carry):
        @pl.when(r + 1 < n)
        def _():
            for k in range(4):
                a_copy(r + 1, k).start()

        ctx = ctx_ref[row0 + r]
        inside = lane < ctx
        cs[0] = jnp.where(inside, tab, pltpu.roll(tab, lax.rem(seq - mb_ref[row0 + r], seq), 1)[:, :1])
        cs[1] = jnp.where(inside, jnp.where(is_cos, 1.0, 0.0), pltpu.roll(tab, ctx - 1, 1))
        lim = jnp.maximum(ii + x * (2 * T), ctx - 1)
        for kb in (1, 2, 3):
            mask[kb - 1] = jnp.where(jj <= lim - kb * T, 0.0, -jnp.inf)

        @pl.when(r > 0)
        def _():
            for cp in kv_copy(r - 1):
                cp.wait()

        for k in range(4):
            project(r, k, True)
        for cp in kv_copy(r):
            cp.start()

        @pl.when(r > 0)
        def _():
            for cp in ct_copy(r - 1):
                cp.wait()

        good = lax.fori_loop(0, HALF_HEADS // UNROLL, fast, jnp.ones((1, 2 * T), F32))

        @pl.when(jnp.min(good) < 0.5)
        def _():
            lax.fori_loop(0, HALF_HEADS, slow, 0)

        for cp in ct_copy(r):
            cp.start()
        return carry

    lax.fori_loop(0, n, row, 0)
    if pn:
        for cp in wd_copy:
            cp.wait()
        for r in range(pn):
            for cp in d_copy(r):
                cp.wait()

        def drow(r, carry):
            do[r] = dense_row(dctx[r], wd[...], da[r], bias_row(bd_ref))
            o_copy(r).start()
            return carry

        lax.fori_loop(0, pn, drow, 0)
        for r in range(pn):
            o_copy(r).wait()
    for cp in kv_copy(n - 1) + ct_copy(n - 1):
        cp.wait()


def dense_kernel(g_ref, mine_ref, theirs_ref, w0_ref, w1_ref, w2_ref, w3_ref, a_ref, b_ref, *rest):
    o_ref = rest[-1]
    w = jnp.concatenate([w0_ref[0], w1_ref[0], w2_ref[0], w3_ref[0]], axis=0)
    o_ref[0] = dense_row(jnp.concatenate([mine_ref[0], theirs_ref[0]], axis=0), w, a_ref[0], bias_row(b_ref))


def solution(mesh):
    sp = mesh.shape["sp"]
    core_swap = [(i, i ^ 1) for i in range(sp)]
    chip_swap = [(i, i ^ 2) for i in range(sp)]
    both_swap = [(i, i ^ 3) for i in range(sp)]

    def local_block(hidden, pos_ids, block_ids, ctx_len, ln_gamma, ln_beta, w_qkv, b_qkv, w_dense, b_dense):
        rows, tok, width = hidden.shape
        seq = tok * sp
        s = lax.axis_index("sp")
        gamma = ln_gamma.astype(F32).reshape(8, width // 8)
        beta = ln_beta.astype(F32).reshape(8, width // 8)
        starts = [sum(CHUNKS[:i]) for i in range(len(CHUNKS))]

        whole = pl.BlockSpec(memory_space=pltpu.VMEM)
        any_ = pl.BlockSpec(memory_space=pl.ANY)
        smem = pl.BlockSpec(memory_space=pltpu.SMEM)
        row_blk = lambda start, shape: pl.BlockSpec((1,) + shape, lambda r, *_: (r + start,) + (0,) * len(shape))
        group_blk = lambda j, shape: pl.BlockSpec(
            (1,) + shape, lambda r, g: (g[j],) + (0,) * len(shape), pipeline_mode=pl.Buffered(1)
        )
        par = pltpu.CompilerParams(dimension_semantics=("arbitrary",), vmem_limit_bytes=67_000_000)

        def ln(start, sizes):
            n = sum(sizes)
            splits = [(sum(sizes[:i]), sz) for i, sz in enumerate(sizes)]
            return pl.pallas_call(
                functools.partial(ln_kernel, splits),
                grid=(n,),
                in_specs=[row_blk(start, (tok, width)), whole, whole],
                out_specs=[
                    pl.BlockSpec((1, tok, width), lambda r, st=st, sz=sz: (jnp.clip(r - st, 0, sz - 1), 0, 0))
                    for st, sz in splits
                ],
                out_shape=[jax.ShapeDtypeStruct((sz, tok, width), BF) for sz in sizes],
                cost_estimate=pl.CostEstimate(flops=n * tok * width * 10, bytes_accessed=n * tok * width * 4, transcendentals=0),
                compiler_params=pltpu.CompilerParams(dimension_semantics=("arbitrary",), vmem_limit_bytes=67_000_000),
                name="ln",
            )(hidden, gamma, beta)

        a_own = ln(0, CHUNKS[:1]) + ln(starts[1], CHUNKS[1:2]) + ln(starts[2], CHUNKS[2:])
        a_chip = [lax.ppermute(a, "sp", chip_swap) for a in a_own]
        a_core = [lax.ppermute(a, "sp", core_swap) for a in a_own]

        last = pos_ids[:, tok - 1]
        got = [last] + [lax.ppermute(last, "sp", pm) for pm in (core_swap, chip_swap, both_swap)]
        m_pos = got[0]
        for k in (1, 2, 3):
            m_pos = jnp.where((s ^ k) == sp - 1, got[k], m_pos)

        inv = ROPE_BASE ** (-jnp.arange(0, 32, 2).astype(F32) / 32)
        ang = jnp.arange(seq, dtype=jnp.int32).astype(F32)[None, :] * inv[:, None]
        tab = jnp.concatenate([jnp.cos(ang), jnp.sin(ang)], axis=0)

        wt = jnp.transpose(w_qkv, (1, 2, 3, 0)).reshape(4, 3 * GRP, width)
        bias = jnp.broadcast_to(b_qkv.astype(F32).reshape(4, 3 * GRP, 1), (4, 3 * GRP, 128))
        wd = w_dense.reshape(4, GRP, width)
        bd = b_dense.astype(F32).reshape(8, width // 8)

        x, c = lax.div(s, 2), lax.rem(s, 2)
        groups = jnp.stack([2 * x + c, 2 * (1 - x) + c, 2 * x + 1 - c, 2 * (1 - x) + 1 - c]).astype(jnp.int32)

        keys = vals = out = mine = theirs = None
        kv_shape = jax.ShapeDtypeStruct((rows, GRP, seq), BF)
        o_shape = jax.ShapeDtypeStruct((rows, tok, width), BF)
        for i, (st, n) in enumerate(zip(starts, CHUNKS)):
            pn = CHUNKS[i - 1] if i else 0
            a_both = lax.ppermute(a_chip[i], "sp", core_swap)
            c_shape = jax.ShapeDtypeStruct((n, HD, tok), BF)
            flops = n * (2 * seq * width * HD * 2 + 2 * tok * 2 * width * HD + HALF_HEADS * 7 * tok * tok * 4 * 256)
            args = [ctx_len, m_pos, tab, bd, wt, bias, wd, a_own[i], a_core[i], a_chip[i], a_both]
            specs = [smem, smem, whole, whole] + [any_] * 7
            if i:
                args += [mine, theirs, a_own[i - 1], keys, vals, out]
                specs += [any_] * 6
            m = max(pn, 1)
            dma = pltpu.SemaphoreType.DMA
            keys, vals, mine, send, out = pl.pallas_call(
                functools.partial(attn_kernel, st, n, starts[i - 1] if i else 0, pn),
                in_specs=specs,
                out_specs=[any_] * 5,
                out_shape=[kv_shape, kv_shape, c_shape, c_shape, o_shape],
                scratch_shapes=[
                    pltpu.VMEM((2, 3 * GRP, width), BF),
                    pltpu.VMEM((2, 3 * GRP, 128), F32),
                    pltpu.VMEM((width, width), BF),
                    pltpu.VMEM((2, 4, tok, width), BF),
                    pltpu.VMEM((HD, seq), BF),
                    pltpu.VMEM((HD, seq), BF),
                    pltpu.VMEM((HD, 2 * tok), BF),
                    pltpu.VMEM((2, HD, tok), BF),
                    pltpu.VMEM((3, tok, 2 * tok), F32),
                    pltpu.VMEM((2, 32, seq), F32),
                    pltpu.VMEM((m, 2 * HD, tok), BF),
                    pltpu.VMEM((m, tok, width), BF),
                    pltpu.VMEM((m, tok, width), BF),
                    dma((2,)),
                    dma((2,)),
                    dma((4,)),
                    dma((2, 4)),
                    dma((2,)),
                    dma((2,)),
                    dma((m, 2)),
                    dma((m,)),
                    dma((m,)),
                ],
                input_output_aliases={14: 0, 15: 1, 16: 4} if i else {},
                cost_estimate=pl.CostEstimate(flops=flops, bytes_accessed=n * 5 * 2**20, transcendentals=0),
                compiler_params=pltpu.CompilerParams(vmem_limit_bytes=67_000_000),
                name="attn",
            )(*args)
            theirs = lax.ppermute(send, "sp", core_swap)

        st, n = starts[-1], CHUNKS[-1]
        out = pl.pallas_call(
            dense_kernel,
            grid_spec=pltpu.PrefetchScalarGridSpec(
                num_scalar_prefetch=1,
                grid=(n,),
                in_specs=[row_blk(0, (HD, tok)), row_blk(0, (HD, tok))]
                + [group_blk(j, (GRP, width)) for j in range(4)]
                + [row_blk(0, (tok, width)), whole, any_],
                out_specs=row_blk(st, (tok, width)),
            ),
            out_shape=o_shape,
            input_output_aliases={9: 0},
            cost_estimate=pl.CostEstimate(flops=n * 2 * tok * width * width, bytes_accessed=n * 2 * 2**20, transcendentals=0),
            compiler_params=par,
            name="dense",
        )(groups, mine, theirs, wd, wd, wd, wd, a_own[-1], bd, out)
        to_out = lambda kv: jnp.transpose(kv.reshape(rows, HALF_HEADS // 2, 64, seq), (0, 3, 1, 2))
        return out, to_out(keys), to_out(vals)

    seq_spec = P("dp", "sp", None)
    row_spec = P("dp", "sp")
    head_spec = P("dp", None, "sp", None)
    rep = P()
    return jax.shard_map(
        local_block,
        mesh=mesh,
        in_specs=(seq_spec, row_spec, row_spec, P("dp"), rep, rep, rep, rep, rep, rep),
        out_specs=(seq_spec, head_spec, head_spec),
        check_vma=False,
    )
```

```python
import functools
import math

import jax
import jax.numpy as jnp
from jax import lax
from jax.experimental import pallas as pl
from jax.experimental.pallas import tpu as pltpu
from jax.sharding import PartitionSpec as P

ALPHA = math.sqrt(56.0)
ROPE_BASE = 10000.0
LN_EPS = 1e-5
BF = jnp.bfloat16
F32 = jnp.float32
T = 256
HALF_HEADS = 8
HD = HALF_HEADS * 64
GRP = HD // 2
CHUNKS = (1, 2, 2, 2, 2, 2, 2, 2, 1)
UNROLL = 4
ATTN_VMEM = 40 * 2**20
BIG = 2.0**60
NT = (((1,), (1,)), ((), ()))
TN = (((0,), (0,)), ((), ()))


def place():
    s = lax.axis_index("sp")
    return lax.div(s, 2), lax.rem(s, 2)


def ln_kernel(n, splits, x_ref, g_ref, b_ref, *refs):
    o_refs, (buf, sem) = refs[:-2], refs[-2:]
    r = pl.program_id(0)
    slot = lax.rem(r, 2)

    def out_copy(row, act):
        for (st, size), o_ref in zip(splits, o_refs):

            @pl.when((row >= st) & (row < st + size))
            def _(o_ref=o_ref, st=st):
                s = lax.rem(row, 2)
                act(pltpu.make_async_copy(buf.at[s], o_ref.at[row - st], sem.at[s]))

    @pl.when(r >= 2)
    def _():
        out_copy(r - 2, lambda cp: cp.wait())

    x = x_ref[0].astype(F32)
    mean = jnp.mean(x, axis=-1, keepdims=True)
    cen = x - mean
    var = jnp.mean(cen * cen, axis=-1, keepdims=True)
    g = g_ref[...].astype(F32)[None, :]
    b = b_ref[...].astype(F32)[None, :]
    buf[slot] = (cen * lax.rsqrt(var + LN_EPS) * g + b).astype(BF)
    out_copy(r, lambda cp: cp.start())

    @pl.when(r == n - 1)
    def _():
        if n > 1:
            out_copy(r - 1, lambda cp: cp.wait())
        out_copy(r, lambda cp: cp.wait())


def rope(x, cos, sin):
    rows, t = x.shape
    x = x.reshape(rows // 64, 2, 2, 16, t)
    u, w = x[:, :, 0], x[:, :, 1]
    return jnp.stack([u * cos - w * sin, w * cos + u * sin], axis=2).reshape(rows, t).astype(BF)


def dense_row(ctx, w, a, b):
    o = lax.dot_general(ctx, w, TN, preferred_element_type=F32)
    return (a.astype(F32) * ALPHA + o + b).astype(BF)


def bias_row(b_ref):
    return jnp.concatenate([b_ref[i : i + 1] for i in range(8)], axis=1)


def attn_kernel(row0, n, prow0, pn, *refs):
    (ctx_ref, mb_ref, tab_ref, bd_ref, w, bias, wd, a0, a1, a2, a3) = refs[:11]
    pm_hbm, pt_hbm, pa_hbm = refs[11:14] if pn else (None,) * 3
    (k_hbm, v_hbm, mine_hbm, send_hbm, o_hbm) = refs[-21:-16]
    (abuf, kt, vt, qt, ct, mask, cs, dctx, da, do) = refs[-16:-6]
    (a_sem, kv_sem, ct_sem, dc_sem, da_sem, do_sem) = refs[-6:]
    x, c = place()
    seq = kt.shape[1]
    g = (2 * x + c, 2 * (1 - x) + c)
    dg = g + (2 * x + 1 - c, 2 * (1 - x) + 1 - c)
    copy = pltpu.make_async_copy

    def a_copy(r, k):
        slot = lax.rem(r, 2)
        return copy((a0, a1, a2, a3)[k].at[r], abuf.at[slot, k], a_sem.at[slot, k])

    def kv_copy(r):
        return (
            copy(kt.at[pl.ds(0, GRP)], k_hbm.at[row0 + r], kv_sem.at[0]),
            copy(vt.at[pl.ds(0, GRP)], v_hbm.at[row0 + r], kv_sem.at[1]),
        )

    def ct_copy(r):
        return (
            copy(ct.at[c], mine_hbm.at[r], ct_sem.at[0]),
            copy(ct.at[1 - c], send_hbm.at[r], ct_sem.at[1]),
        )

    def d_copy(r):
        return (
            copy(pm_hbm.at[r], dctx.at[r, pl.ds(0, HD)], dc_sem.at[r, 0]),
            copy(pt_hbm.at[r], dctx.at[r, pl.ds(HD, HD)], dc_sem.at[r, 1]),
            copy(pa_hbm.at[r], da.at[r], da_sem.at[r]),
        )

    def o_copy(r):
        return copy(do.at[r], o_hbm.at[prow0 + r], do_sem.at[r])

    for k in range(4):
        a_copy(0, k).start()
    for r in range(pn):
        for cp in d_copy(r):
            cp.start()

    tab = tab_ref[...]
    lane = lax.broadcasted_iota(jnp.int32, (1, seq), 1)
    is_cos = lax.broadcasted_iota(jnp.int32, (32, 1), 0) < 16
    jj = lax.broadcasted_iota(jnp.int32, (T, 2 * T), 0)
    ii = lax.broadcasted_iota(jnp.int32, (1, 2 * T), 1)

    def part(ref, t, lanes):
        return jnp.concatenate(
            [ref[gj].reshape(4, 192, lanes)[:, t * 64 : t * 64 + 64].reshape(GRP, lanes) for gj in g], axis=0
        )

    def project(r, k):
        own = k < 2
        blk = 2 * (x if own else 1 - x) + (c if k % 2 == 0 else 1 - c)
        off = pl.multiple_of(blk * T, T)
        a = abuf[lax.rem(r, 2), k]
        cos = jnp.stack([cs[0, :16, pl.ds(off, T)], cs[1, :16, pl.ds(off, T)]], axis=0)[None]
        sin = jnp.stack([cs[0, 16:, pl.ds(off, T)], cs[1, 16:, pl.ds(off, T)]], axis=0)[None]

        def rows_of(t):
            z = lax.dot_general(part(w, t, 1024), a, NT, preferred_element_type=F32)
            b = part(bias, t, 128)
            return (z + jnp.concatenate([b, b], axis=1)).astype(BF)

        kt[:, pl.ds(off, T)] = rope(rows_of(1).astype(F32), cos, sin)
        vt[:, pl.ds(off, T)] = rows_of(2)
        if own:
            qoff = pl.multiple_of((c if k == 0 else 1 - c) * T, T)
            qt[:, pl.ds(qoff, T)] = rope(rows_of(0).astype(F32), cos, sin) * jnp.asarray(0.125, BF)

    def scores(ho, kb):
        k_blk = kt[pl.ds(ho, 64), kb * T : (kb + 1) * T]
        q = qt[pl.ds(ho, 64), :] if kb < 3 else qt[pl.ds(ho, 64), T:]
        st = lax.dot_general(k_blk, q, TN, preferred_element_type=F32)
        if kb == 0:
            return st
        return st + (mask[kb - 1] if kb < 3 else mask[2, :, T:])

    def finish(ho, es, l):
        pa = jnp.concatenate([e[:, :T] for e in es[:3]], axis=0)
        pb = jnp.concatenate([e[:, T:] for e in es[:3]] + [es[3]], axis=0)
        oa = jnp.dot(vt[pl.ds(ho, 64), : 3 * T], pa, preferred_element_type=F32)
        ob = jnp.dot(vt[pl.ds(ho, 64), :], pb, preferred_element_type=F32)
        inv = 1.0 / l
        ct[0, pl.ds(ho, 64)] = (oa * inv[:, :T]).astype(BF)
        ct[1, pl.ds(ho, 64)] = (ob * inv[:, T:]).astype(BF)
        return oa, ob

    def total(es):
        l = jnp.sum(es[0], axis=0, keepdims=True)
        for e in es[1:3]:
            l = l + jnp.sum(e, axis=0, keepdims=True)
        return jnp.concatenate([l[:, :T], l[:, T:] + jnp.sum(es[3], axis=0, keepdims=True)], axis=1)

    def fast(i, good):
        for u in range(UNROLL):
            ho = pl.multiple_of(i * (UNROLL * 64) + u * 64, 64)
            es = [jnp.exp(scores(ho, kb)) for kb in range(4)]
            l = total(es)
            oa, ob = finish(ho, [e.astype(BF) for e in es], l)
            top = jnp.concatenate(
                [jnp.max(jnp.abs(oa), axis=0, keepdims=True), jnp.max(jnp.abs(ob), axis=0, keepdims=True)], axis=1
            )
            ok = (l >= 1.0 / BIG) & (l <= BIG) & (top <= BIG * BIG)
            good = jnp.minimum(good, jnp.where(ok, 1.0, 0.0))
        return good

    def slow(h, carry):
        ho = pl.multiple_of(h * 64, 64)
        ss = [scores(ho, kb) for kb in range(4)]
        m = jnp.max(ss[0], axis=0, keepdims=True)
        for st in ss[1:3]:
            m = jnp.maximum(m, jnp.max(st, axis=0, keepdims=True))
        mb = jnp.maximum(m[:, T:], jnp.max(ss[3], axis=0, keepdims=True))
        m = jnp.concatenate([m[:, :T], mb], axis=1)
        es = [jnp.exp(st - m) for st in ss[:3]] + [jnp.exp(ss[3] - mb)]
        finish(ho, [e.astype(BF) for e in es], total(es))
        return carry

    def row(r, carry):
        @pl.when(r + 1 < n)
        def _():
            for k in range(4):
                a_copy(r + 1, k).start()

        @pl.when(r > 0)
        def _():
            for cp in kv_copy(r - 1) + ct_copy(r - 1):
                cp.wait()

        for k in range(4):
            a_copy(r, k).wait()

        ctx = ctx_ref[row0 + r]
        inside = lane < ctx
        cs[0] = jnp.where(inside, tab, pltpu.roll(tab, lax.rem(seq - mb_ref[row0 + r], seq), 1)[:, :1])
        cs[1] = jnp.where(inside, jnp.where(is_cos, 1.0, 0.0), pltpu.roll(tab, ctx - 1, 1))
        lim = jnp.maximum(ii + x * (2 * T), ctx - 1)
        for kb in (1, 2):
            mask[kb - 1] = jnp.where(jj <= lim - kb * T, 0.0, -jnp.inf)
        mask[2, :, T:] = jnp.where(jj[:, T:] <= lim[:, T:] - 3 * T, 0.0, -jnp.inf)
        for k in range(4):
            project(r, k)
        for cp in kv_copy(r):
            cp.start()

        good = lax.fori_loop(0, HALF_HEADS // UNROLL, fast, jnp.ones((1, 2 * T), F32))

        @pl.when(jnp.min(good) < 0.5)
        def _():
            lax.fori_loop(0, HALF_HEADS, slow, 0)

        for cp in ct_copy(r):
            cp.start()
        return carry

    lax.fori_loop(0, n, row, 0)
    if pn:
        for r in range(pn):
            for cp in d_copy(r):
                cp.wait()

        def drow(r, carry):
            do[r] = dense_row(dctx[r], jnp.concatenate([wd[gj] for gj in dg], axis=0), da[r], bias_row(bd_ref))
            o_copy(r).start()
            return carry

        lax.fori_loop(0, pn, drow, 0)
        for r in range(pn):
            o_copy(r).wait()
    for cp in kv_copy(n - 1) + ct_copy(n - 1):
        cp.wait()


def dense_kernel(mine_ref, theirs_ref, wd_ref, a_ref, b_ref, *rest):
    o_ref = rest[-1]
    x, c = place()
    w = jnp.concatenate([wd_ref[g] for g in (2 * x + c, 2 * (1 - x) + c, 2 * x + 1 - c, 2 * (1 - x) + 1 - c)], axis=0)
    o_ref[0] = dense_row(jnp.concatenate([mine_ref[0], theirs_ref[0]], axis=0), w, a_ref[0], bias_row(b_ref))


def solution(mesh):
    sp = mesh.shape["sp"]
    core_swap = [(i, i ^ 1) for i in range(sp)]
    chip_swap = [(i, i ^ 2) for i in range(sp)]
    both_swap = [(i, i ^ 3) for i in range(sp)]

    def local_block(hidden, pos_ids, block_ids, ctx_len, ln_gamma, ln_beta, w_qkv, b_qkv, w_dense, b_dense):
        rows, tok, width = hidden.shape
        seq = tok * sp
        s = lax.axis_index("sp")
        starts = [sum(CHUNKS[:i]) for i in range(len(CHUNKS))]

        whole = pl.BlockSpec(memory_space=pltpu.VMEM)
        hbm = pl.BlockSpec(memory_space=pltpu.HBM)
        smem = pl.BlockSpec(memory_space=pltpu.SMEM)
        row_blk = lambda start, shape: pl.BlockSpec((1,) + shape, lambda r, *_: (r + start,) + (0,) * len(shape))
        par = pltpu.CompilerParams(dimension_semantics=("arbitrary",), vmem_limit_bytes=ATTN_VMEM)

        def ln(start, sizes):
            n = sum(sizes)
            splits = [(sum(sizes[:i]), sz) for i, sz in enumerate(sizes)]
            return pl.pallas_call(
                functools.partial(ln_kernel, n, splits),
                grid=(n,),
                in_specs=[row_blk(start, (tok, width)), whole, whole],
                out_specs=[hbm] * len(sizes),
                scratch_shapes=[pltpu.VMEM((2, tok, width), BF), pltpu.SemaphoreType.DMA((2,))],
                out_shape=[jax.ShapeDtypeStruct((sz, tok, width), BF) for sz in sizes],
                cost_estimate=pl.CostEstimate(flops=n * tok * width * 10, bytes_accessed=n * tok * width * 4, transcendentals=0),
                compiler_params=pltpu.CompilerParams(dimension_semantics=("arbitrary",), vmem_limit_bytes=67_000_000),
                name="ln",
            )(hidden, ln_gamma, ln_beta)

        a_own = ln(0, CHUNKS[:1]) + ln(starts[1], CHUNKS[1:2]) + ln(starts[2], CHUNKS[2:])
        a_chip = [lax.ppermute(a, "sp", chip_swap) for a in a_own]
        a_core = [lax.ppermute(a, "sp", core_swap) for a in a_own]

        last = pos_ids[:, tok - 1]
        got = [last] + [lax.ppermute(last, "sp", pm) for pm in (core_swap, chip_swap, both_swap)]
        m_pos = got[0]
        for k in (1, 2, 3):
            m_pos = jnp.where((s ^ k) == sp - 1, got[k], m_pos)

        inv = ROPE_BASE ** (-jnp.arange(0, 32, 2).astype(F32) / 32)
        ang = jnp.arange(seq, dtype=jnp.int32).astype(F32)[None, :] * inv[:, None]
        tab = jnp.concatenate([jnp.cos(ang), jnp.sin(ang)], axis=0)

        wt = jnp.transpose(w_qkv, (1, 2, 3, 0)).reshape(4, 3 * GRP, width)
        bias = jnp.broadcast_to(b_qkv.astype(F32).reshape(4, 3 * GRP, 1), (4, 3 * GRP, 128))
        wd = w_dense.reshape(4, GRP, width)
        bd = b_dense.astype(F32).reshape(8, width // 8)

        keys = vals = out = mine = theirs = None
        kv_shape = jax.ShapeDtypeStruct((rows, GRP, seq), BF)
        o_shape = jax.ShapeDtypeStruct((rows, tok, width), BF)
        for i, (st, n) in enumerate(zip(starts, CHUNKS)):
            pn = CHUNKS[i - 1] if i else 0
            a_both = lax.ppermute(a_chip[i], "sp", core_swap)
            c_shape = jax.ShapeDtypeStruct((n, HD, tok), BF)
            flops = n * (2 * seq * width * HD * 2 + 2 * tok * 2 * width * HD + HALF_HEADS * 7 * tok * tok * 4 * 256)
            args = [ctx_len, m_pos, tab, bd, wt, bias, wd, a_own[i], a_core[i], a_chip[i], a_both]
            specs = [smem, smem] + [whole] * 5 + [hbm] * 4
            if i:
                args += [mine, theirs, a_own[i - 1], keys, vals, out]
                specs += [hbm] * 6
            m = max(pn, 1)
            dma = pltpu.SemaphoreType.DMA
            keys, vals, mine, send, out = pl.pallas_call(
                functools.partial(attn_kernel, st, n, starts[i - 1] if i else 0, pn),
                in_specs=specs,
                out_specs=[hbm] * 5,
                out_shape=[kv_shape, kv_shape, c_shape, c_shape, o_shape],
                scratch_shapes=[
                    pltpu.VMEM((2, 4, tok, width), BF),
                    pltpu.VMEM((HD, seq), BF),
                    pltpu.VMEM((HD, seq), BF),
                    pltpu.VMEM((HD, 2 * tok), BF),
                    pltpu.VMEM((2, HD, tok), BF),
                    pltpu.VMEM((3, tok, 2 * tok), F32),
                    pltpu.VMEM((2, 32, seq), F32),
                    pltpu.VMEM((m, 2 * HD, tok), BF),
                    pltpu.VMEM((m, tok, width), BF),
                    pltpu.VMEM((m, tok, width), BF),
                    dma((2, 4)),
                    dma((2,)),
                    dma((2,)),
                    dma((m, 2)),
                    dma((m,)),
                    dma((m,)),
                ],
                input_output_aliases={14: 0, 15: 1, 16: 4} if i else {},
                cost_estimate=pl.CostEstimate(flops=flops, bytes_accessed=n * 5 * 2**20, transcendentals=0),
                compiler_params=pltpu.CompilerParams(vmem_limit_bytes=ATTN_VMEM),
                name="attn",
            )(*args)
            theirs = lax.ppermute(send, "sp", core_swap)

        st, n = starts[-1], CHUNKS[-1]
        out = pl.pallas_call(
            dense_kernel,
            grid=(n,),
            in_specs=[row_blk(0, (HD, tok)), row_blk(0, (HD, tok)), whole, row_blk(0, (tok, width)), whole, hbm],
            out_specs=row_blk(st, (tok, width)),
            out_shape=o_shape,
            input_output_aliases={5: 0},
            cost_estimate=pl.CostEstimate(flops=n * 2 * tok * width * width, bytes_accessed=n * 2 * 2**20, transcendentals=0),
            compiler_params=par,
            name="dense",
        )(mine, theirs, wd, a_own[-1], bd, out)
        to_out = lambda kv: jnp.transpose(kv.reshape(rows, HALF_HEADS // 2, 64, seq), (0, 3, 1, 2))
        return out, to_out(keys), to_out(vals)

    seq_spec = P("dp", "sp", None)
    row_spec = P("dp", "sp")
    head_spec = P("dp", None, "sp", None)
    rep = P()
    return jax.shard_map(
        local_block,
        mesh=mesh,
        in_specs=(seq_spec, row_spec, row_spec, P("dp"), rep, rep, rep, rep, rep, rep),
        out_specs=(seq_spec, head_spec, head_spec),
        check_vma=False,
    )
```
